8 devices in a mesh: dp: 2 (over y, z), sp: 4 (over x, core).
Axes of the slice: x: 2, y: 2, z: 1, core: 2. Of those that a mesh axis runs over, the one named last changes fastest.
Arguments:
- x: bfloat16 [16384, 2048], P(('dp', 'sp')), parts along dimension 0
- gain: bfloat16 [2048], replicated
- wq: bfloat16 [2048, 2048], P('sp')
- wk: bfloat16 [2048, 2048], P('sp')
- wv: bfloat16 [2048, 2048], P('sp')
- wo: bfloat16 [2048, 2048], P('sp')
Outputs:
- output: bfloat16 [16384, 2048], P(('dp', 'sp')), parts along dimension 0
There are 2 independent parts. The reference program is written for one: setup_inputs(seed, part) draws one part's arguments, and reference() takes and returns one part's arrays. A program takes and returns all parts, laid end to end along the dimension named above; an argument that names none is the same for every part.
All inputs are finite; a program needn't handle non-finite values.
Results may differ from the reference program's by a relative error of at most 0.012.
Values are sent between devices in bfloat16 or wider.
A program may use at most 2 GiB of HBM per device.

```python
import jax
import jax.numpy as jnp
from jax import lax

ROWS = 8192
D = 2048
HEADS = 8
KV_HEADS = 8
HEAD = 256
THETA = 10000


def setup_inputs(seed: int = 0, part: int = 0) -> dict:
    kx, kn, kq, kk, kv, ko = jax.random.split(jax.random.key(seed), 6)

    def weights(key, rows, columns):
        return jax.random.normal(key, (rows, columns), jnp.float32) * rows**-0.5

    drawn = {
        "x": jax.random.normal(jax.random.fold_in(kx, part), (ROWS, D), jnp.float32),
        "gain": 1 + 0.1 * jax.random.normal(kn, (D,), jnp.float32),
        "wq": 2 * weights(kq, D, HEADS * HEAD),
        "wk": 2 * weights(kk, D, KV_HEADS * HEAD),
        "wv": 4 * weights(kv, D, KV_HEADS * HEAD),
        "wo": weights(ko, HEADS * HEAD, D),
    }
    return {k: v.astype(jnp.bfloat16) for k, v in drawn.items()}


def normed(x, gain):
    wide = x.astype(jnp.float32)
    scale = lax.rsqrt(jnp.mean(wide * wide, -1, keepdims=True) + 1e-6)
    return (wide * scale * gain.astype(jnp.float32)).astype(jnp.bfloat16)


def turned(t, place, theta):
    half = t.shape[-1] // 2
    angle = place.astype(jnp.float32)[:, None] * theta ** (-jnp.arange(half, dtype=jnp.float32) / half)
    cos, sin = jnp.cos(angle)[:, None], jnp.sin(angle)[:, None]
    a, b = t[..., :half].astype(jnp.float32), t[..., half:].astype(jnp.float32)
    return jnp.concatenate([a * cos - b * sin, b * cos + a * sin], -1).astype(jnp.bfloat16)


def matmul(a, w):
    return jnp.dot(a, w, preferred_element_type=jnp.float32).astype(jnp.bfloat16)


def einsum(form, a, b):
    return jnp.einsum(form, a.astype(jnp.float32), b.astype(jnp.float32))


def attention(q, k, v):
    scores = einsum("tgsd,ugd->gstu", q, k) * q.shape[-1] ** -0.5
    token = jnp.arange(q.shape[0])
    scores = jnp.where(token[:, None] >= token, scores, -jnp.inf)
    weights = jax.nn.softmax(scores, -1).astype(jnp.bfloat16)
    return einsum("gstu,ugd->tgsd", weights, v).astype(jnp.bfloat16)


def reference(x, gain, wq, wk, wv, wo):
    a, place = normed(x, gain), jnp.arange(ROWS)
    q = turned(matmul(a, wq).reshape(ROWS, HEADS, HEAD), place, THETA).reshape(ROWS, KV_HEADS, -1, HEAD)
    k = turned(matmul(a, wk).reshape(ROWS, KV_HEADS, HEAD), place, THETA)
    v = matmul(a, wv).reshape(ROWS, KV_HEADS, HEAD)
    seen = attention(q, k, v).reshape(ROWS, HEADS * HEAD)
    return (x.astype(jnp.float32) + jnp.dot(seen, wo, preferred_element_type=jnp.float32)).astype(jnp.bfloat16)
```

```python
import functools

import jax
import jax.numpy as jnp
from jax import lax
from jax.experimental import pallas as pl
from jax.experimental.pallas import tpu as pltpu
from jax.sharding import PartitionSpec as P


HEAD = 256
HEADS = 8
THETA = 10000
NEG = -1e30
HIDDEN = 2 * NEG
LOG2E = 1.4426950408889634
VMEM = 60 * 2**20
AXES = ("dp", "sp")
CHUNKS = (1024, 512, 512)


def _pairs(to, only=lambda y, x, c: True):
    number = lambda y, x, c: y * 4 + x * 2 + c
    return [(number(*p), number(*to(*p))) for p in [(y, x, c) for y in (0, 1) for x in (0, 1) for c in (0, 1)] if only(*p)]


ACROSS_X = _pairs(lambda y, x, c: (y, 1 - x, c))
ACROSS_Y = _pairs(lambda y, x, c: (1 - y, x, c))
TO_CORE = _pairs(lambda y, x, c: (y, x, 1 - c))
FORWARD = _pairs(lambda y, x, c: (y, 1, c), lambda y, x, c: x == 0)
SECOND_TO_CORE = _pairs(lambda y, x, c: (y, x, 1 - c), lambda y, x, c: x == 1)


def _send(t, pairs):
    return lax.ppermute(t, AXES, pairs)


def _dot(a, b, ca, cb):
    return lax.dot_general(a, b, (((ca,), (cb,)), ((), ())), preferred_element_type=jnp.float32)


def normed(x, gain):
    wide = x.astype(jnp.float32)
    scale = lax.rsqrt(jnp.mean(wide * wide, -1, keepdims=True) + 1e-6)
    return (wide * scale * gain.astype(jnp.float32)).astype(jnp.bfloat16)


def _place(s_ref, pieces, w_s, unit):
    for n, piece in enumerate(pieces):
        w_s[pl.ds(pl.multiple_of(s_ref[n] * unit, unit), piece.shape[0]), :] = piece[...]


def _project(s_ref, a_ref, b_ref, *rest, turn, unit, half):
    rest = list(rest)
    pieces, rest = rest[:6], rest[6:]
    if turn:
        cos_ref, sin_ref = rest[:2]
        rest = rest[2:]
    o_ref, w_s = rest
    i = pl.program_id(0)

    @pl.when(i == 0)
    def _():
        _place(s_ref, pieces, w_s, unit)

    def make(from_ref):
        heads = o_ref.shape[0]
        product = lambda h: _dot(from_ref[...], w_s[:, h * HEAD : (h + 1) * HEAD], 1, 0)
        ahead = product(0)
        for h in range(heads):
            t = ahead.astype(jnp.bfloat16)
            if h + 1 < heads:
                ahead = product(h + 1)
            if turn:
                t = t.astype(jnp.float32)
                a, b = t[:, : HEAD // 2], t[:, HEAD // 2 :]
                cos, sin = cos_ref[...], sin_ref[...]
                o_ref[h, :, : HEAD // 2] = (a * cos - b * sin).astype(o_ref.dtype)
                o_ref[h, :, HEAD // 2 :] = (b * cos + a * sin).astype(o_ref.dtype)
            else:
                o_ref[h] = t.T

    pl.when(i < half)(lambda: make(a_ref))
    pl.when(i >= half)(lambda: make(b_ref))


def project(a, b, weight, core, tables, places, targets, rows=512):
    pieces, at = weight
    d = a.shape[1]
    heads = HEADS // 2
    unit = d // 8
    tokens = a.shape[0] + b.shape[0]
    half = a.shape[0] // rows
    steps = 2 * half
    turn = tables is not None
    scalars = jnp.concatenate([at, jnp.stack([core]), places, targets]).astype(jnp.int32)
    specs = [
        pl.BlockSpec((rows, d), lambda i, s: (jnp.minimum(i, half - 1), 0)),
        pl.BlockSpec((rows, d), lambda i, s: (jnp.maximum(i - half, 0), 0)),
    ]
    specs += [pl.BlockSpec((p.shape[0], heads * HEAD), lambda i, s: (0, s[6])) for p in pieces]
    given = [a, b, *pieces]
    if turn:
        specs += [pl.BlockSpec((rows, HEAD // 2), lambda i, s: (s[7 + i], 0))] * 2
        given += tables
        out = jax.ShapeDtypeStruct((heads, tokens, HEAD), jnp.bfloat16)
        out_spec = pl.BlockSpec((heads, rows, HEAD), lambda i, s: (0, s[7 + steps + i], 0))
    else:
        out = jax.ShapeDtypeStruct((heads, HEAD, tokens), jnp.bfloat16)
        out_spec = pl.BlockSpec((heads, HEAD, rows), lambda i, s: (0, 0, s[7 + steps + i]))
    return pl.pallas_call(
        functools.partial(_project, turn=turn, unit=unit, half=half),
        grid_spec=pltpu.PrefetchScalarGridSpec(
            num_scalar_prefetch=1,
            grid=(steps,),
            in_specs=specs,
            out_specs=out_spec,
            scratch_shapes=[pltpu.VMEM((d, heads * HEAD), jnp.bfloat16)],
        ),
        out_shape=out,
        compiler_params=pltpu.CompilerParams(dimension_semantics=("arbitrary",), vmem_limit_bytes=VMEM),
        cost_estimate=pl.CostEstimate(flops=2 * tokens * d * heads * HEAD, transcendentals=0, bytes_accessed=4 * tokens * d),
    )(scalars, *given)


def _finish(s_ref, a_ref, b_ref, x_ref, *rest, unit):
    pieces, (o_ref, w_s) = rest[:6], rest[6:]

    @pl.when(pl.program_id(0) == 0)
    def _():
        _place(s_ref, pieces, w_s, unit)

    seen = jnp.concatenate([a_ref[...], b_ref[...]], axis=1)
    wide = 512
    for n in range(0, o_ref.shape[1], wide):
        y = _dot(seen, w_s[:, n : n + wide], 1, 0)
        o_ref[:, n : n + wide] = (x_ref[:, n : n + wide].astype(jnp.float32) + y).astype(o_ref.dtype)


def finish(a, b, x, weight, core, rows=512):
    pieces, at = weight
    tokens, d = x.shape
    unit = d // 8
    at = jnp.where(at // 4 == core, 0, 4) + at % 4
    return pl.pallas_call(
        functools.partial(_finish, unit=unit),
        grid_spec=pltpu.PrefetchScalarGridSpec(
            num_scalar_prefetch=1,
            grid=(tokens // rows,),
            in_specs=[pl.BlockSpec((rows, d // 2), lambda i, s: (i, 0))] * 2
            + [pl.BlockSpec((rows, d), lambda i, s: (i, 0))]
            + [pl.BlockSpec(p.shape, lambda i, s: (0, 0)) for p in pieces],
            out_specs=pl.BlockSpec((rows, d), lambda i, s: (i, 0)),
            scratch_shapes=[pltpu.VMEM((d, d), jnp.bfloat16)],
        ),
        out_shape=jax.ShapeDtypeStruct(x.shape, x.dtype),
        compiler_params=pltpu.CompilerParams(dimension_semantics=("arbitrary",), vmem_limit_bytes=VMEM),
        cost_estimate=pl.CostEstimate(flops=2 * tokens * d * d, transcendentals=0, bytes_accessed=6 * tokens * d),
    )(at.astype(jnp.int32), a, b, x, *pieces)


def _attend(n_ref, q_ref, k_ref, v_ref, *rest, diagonal, carried, final, bq, bk, wide):
    rest = list(rest)
    if carried:
        mix_in, top_in = rest[:2]
        rest = rest[2:]
    outs, (mix_s, top_s) = rest[:-2], rest[-2:]
    iq, blocks = pl.program_id(1), pl.num_programs(1)
    e = HEAD**-0.5 * LOG2E
    strips = range(0, bq, wide)
    if carried:
        mix_s[...] = mix_in[0]
        top_s[...] = top_in[0]
    else:
        mix_s[...] = jnp.zeros_like(mix_s)
        top_s[...] = jnp.full(top_s.shape, NEG, jnp.float32)

    def run(units):
        scores, weights = {}, {}
        for t in range(len(units) + 2):
            if t < len(units):
                at, first, keys, _ = units[t]
                scores[t] = _dot(k_ref[0, pl.ds(first, keys), :], q_ref[0, at : at + wide, :], 1, 1)
            if 0 <= t - 1 < len(units):
                at, first, keys, masked = units[t - 1]
                s = scores.pop(t - 1)
                if masked:
                    low = s[keys - wide :]
                    low = jnp.where(lax.broadcasted_iota(jnp.int32, low.shape, 1) >= lax.broadcasted_iota(jnp.int32, low.shape, 0), low, HIDDEN)
                    s = low if keys == wide else jnp.concatenate([s[: keys - wide], low], axis=0)
                old = top_s[:, at : at + wide]
                top = jnp.maximum(old, s.max(axis=0, keepdims=True))
                top_s[:, at : at + wide] = top
                weights[t - 1] = jnp.exp2((s - top) * e).astype(jnp.bfloat16), jnp.exp2((old - top) * e)
            if 0 <= t - 2:
                at, first, keys, _ = units[t - 2]
                p, keep = weights.pop(t - 2)
                values = jnp.concatenate([v_ref[0, :, pl.ds(first, keys)], jnp.ones((8, keys), jnp.bfloat16)], axis=0)
                mix_s[:, at : at + wide] = mix_s[:, at : at + wide] * keep + _dot(values, p, 1, 0)

    def whole(j, _):
        run([(at, pl.multiple_of(j * bk, bk), bk, False) for at in strips])

    lax.fori_loop(0, iq * (bq // bk) if diagonal else n_ref[0], whole, None)
    if diagonal:
        run([(at, pl.multiple_of(iq * bq, bq), at + wide, True) for at in reversed(strips)])
    if final:

        def put(o_ref):
            o_ref[...] = (mix_s[:HEAD, :] * (1 / mix_s[HEAD : HEAD + 1, :])).T.astype(o_ref.dtype)

        pl.when(iq < blocks // 2)(lambda: put(outs[0]))
        pl.when(iq >= blocks // 2)(lambda: put(outs[1]))
    else:
        outs[0][0] = mix_s[...]
        outs[1][0] = top_s[...]


def attend(q, k, v, count, core, state=None, *, diagonal, final, bq=2048, bk=2048, wide=256):
    heads, queries, d = q.shape
    keys = k.shape[1]
    bk = min(bk, keys)
    blocks = queries // bq
    half = blocks // 2

    def block(iq, s):
        return jnp.where(iq < half, (1 - s[1]) * half + iq, s[1] * half + iq - half) if final else iq

    states = [
        pl.BlockSpec((1, HEAD + 8, bq), lambda ih, iq, s: (ih, 0, block(iq, s))),
        pl.BlockSpec((1, 1, bq), lambda ih, iq, s: (ih, 0, block(iq, s))),
    ]
    specs = [
        pl.BlockSpec((1, bq, d), lambda ih, iq, s: (ih, block(iq, s), 0)),
        pl.BlockSpec((1, keys, d), lambda ih, iq, s: (ih, 0, 0)),
        pl.BlockSpec((1, d, keys), lambda ih, iq, s: (ih, 0, 0)),
    ]
    given = [q, k, v]
    if state is not None:
        given += state
        specs += states
    if final:
        outs = [
            pl.BlockSpec((bq, d), lambda ih, iq, s: (jnp.minimum(iq, half - 1), ih)),
            pl.BlockSpec((bq, d), lambda ih, iq, s: (jnp.maximum(iq - half, 0), ih)),
        ]
        shapes = [jax.ShapeDtypeStruct((queries // 2, heads * d), jnp.bfloat16)] * 2
    else:
        outs = states
        shapes = [jax.ShapeDtypeStruct((heads, HEAD + 8, queries), jnp.float32), jax.ShapeDtypeStruct((heads, 1, queries), jnp.float32)]
    scores = heads * queries * keys // (2 if diagonal else 1)
    return pl.pallas_call(
        functools.partial(_attend, diagonal=diagonal, carried=state is not None, final=final, bq=bq, bk=bk, wide=wide),
        grid_spec=pltpu.PrefetchScalarGridSpec(
            num_scalar_prefetch=1,
            grid=(heads, blocks),
            in_specs=specs,
            out_specs=outs,
            scratch_shapes=[pltpu.VMEM((HEAD + 8, bq), jnp.float32), pltpu.VMEM((1, bq), jnp.float32)],
        ),
        out_shape=shapes,
        compiler_params=pltpu.CompilerParams(dimension_semantics=("arbitrary", "arbitrary"), vmem_limit_bytes=VMEM),
        cost_estimate=pl.CostEstimate(flops=4 * scores * d, transcendentals=scores, bytes_accessed=sum(t.size * t.dtype.itemsize for t in given)),
    )(jnp.stack([count // bk, core]).astype(jnp.int32), *given)


def solution(mesh):
    def step(x, gain, wq, wk, wv, wo):
        own, _ = x.shape
        y, sp = lax.axis_index("dp"), lax.axis_index("sp")
        chip, core = sp // 2, sp % 2
        rows = 512
        per = own // rows

        def cross(w):
            size = w.shape[0] // 2
            part = lax.dynamic_slice_in_dim(w, y * size, size)
            return _send(part, ACROSS_X)

        mine, far_at, far_other = 2 * (2 * chip + core), 2 * (2 * (1 - chip) + core), 2 * (2 * (1 - chip) + 1 - core)
        at_w = jnp.stack([mine, 2 * (2 * chip + 1 - core), far_at + y, far_at + 1 - y, far_other + y, far_other + 1 - y])

        def gather(w, there, other):
            return [w, _send(w, TO_CORE), there, other, _send(there, TO_CORE), _send(other, TO_CORE)], at_w

        after = lax.optimization_barrier

        there = [cross(w) for w in (wk, wv, wq, wo)]
        a = normed(x, gain)
        b = _send(a, TO_CORE)
        other = [_send(t, ACROSS_Y) for t in there[:2]]
        wk = gather(wk, there[0], other[0])
        far, at = [], [sum(CHUNKS[:n]) for n in range(len(CHUNKS))]
        for first, size in zip(at, CHUNKS):
            part = lax.slice_in_dim(a, first, first + size)
            far.append(_send(part, FORWARD))

        half = HEAD // 2
        place = jnp.arange(4 * own)
        angle = place.astype(jnp.float32)[:, None] * THETA ** (-jnp.arange(half, dtype=jnp.float32) / half)
        tables = [jnp.cos(angle), jnp.sin(angle)]

        step_no = jnp.arange(2 * per)
        targets = jnp.where(step_no < per, core * per + step_no, (1 - core) * per + step_no - per)
        places = 2 * chip * per + targets
        k = project(a, b, wk, core, tables, places, targets)
        there[2], other[1], k = after((there[2], other[1], k))
        wv = gather(wv, there[1], other[1])
        other.append(_send(there[2], ACROSS_Y))
        v = project(a, b, wv, core, None, places, targets)
        there[3], other[2], v = after((there[3], other[2], v))
        wq = gather(wq, there[2], other[2])
        other.append(_send(there[3], ACROSS_Y))
        q = project(a, b, wq, core, tables, places, targets)
        far[0], q, k, v, other[3] = after((far[0], q, k, v, other[3]))
        wo = gather(wo, there[3], other[3])
        near = _send(far[0], SECOND_TO_CORE)
        state = attend(q, k, v, jnp.int32(0), core, diagonal=True, final=False)
        for n, first in enumerate(at):
            size = CHUNKS[n]
            blocks = size // rows
            if n + 1 < len(at):
                if n == 0:
                    wo[0][1], wo[0][4], wo[0][5], state = after((wo[0][1], wo[0][4], wo[0][5], state))
                state, near, far[n + 1] = after((state, near, far[n + 1]))
                later = _send(far[n + 1], SECOND_TO_CORE)
            else:
                state, near = after((state, near))
                later = None
            step_no = jnp.arange(2 * blocks)
            places = jnp.where(step_no < blocks, core * per + step_no, (1 - core) * per + step_no - blocks) + first // rows
            k = project(far[n], near, wk, core, tables, places, step_no)
            v = project(far[n], near, wv, core, None, places, step_no)
            state = attend(q, k, v, 2 * size * chip, core, state, diagonal=False, final=n == len(at) - 1)
            near = later
        theirs, mine = state
        return finish(mine, _send(theirs, TO_CORE), x, wo, core)

    tokens, whole = P(AXES, None), P("sp", None)

    return jax.shard_map(
        step,
        mesh=mesh,
        in_specs=(tokens, P(None), whole, whole, whole, whole),
        out_specs=tokens,
        check_vma=False,
    )
```

```python
import functools

import jax
import jax.numpy as jnp
from jax import lax
from jax.experimental import pallas as pl
from jax.experimental.pallas import tpu as pltpu
from jax.sharding import PartitionSpec as P


HEAD = 256
HEADS = 8
THETA = 10000
NEG = -1e30
HIDDEN = 2 * NEG
LOG2E = 1.4426950408889634
ROOM = 40.0
MOST = 8192.0
VMEM = 60 * 2**20
AXES = ("dp", "sp")
CHUNKS = (1024, 1024)


def _pairs(to, only=lambda y, x, c: True):
    number = lambda y, x, c: y * 4 + x * 2 + c
    return [(number(*p), number(*to(*p))) for p in [(y, x, c) for y in (0, 1) for x in (0, 1) for c in (0, 1)] if only(*p)]


ACROSS_X = _pairs(lambda y, x, c: (y, 1 - x, c))
ACROSS_Y = _pairs(lambda y, x, c: (1 - y, x, c))
TO_CORE = _pairs(lambda y, x, c: (y, x, 1 - c))
FORWARD = _pairs(lambda y, x, c: (y, 1, c), lambda y, x, c: x == 0)
SECOND_TO_CORE = _pairs(lambda y, x, c: (y, x, 1 - c), lambda y, x, c: x == 1)


def _send(t, pairs):
    return lax.ppermute(t, AXES, pairs)


def _dot(a, b, ca, cb):
    return lax.dot_general(a, b, (((ca,), (cb,)), ((), ())), preferred_element_type=jnp.float32)


def normed(x, gain):
    wide = x.astype(jnp.float32)
    scale = lax.rsqrt(jnp.mean(wide * wide, -1, keepdims=True) + 1e-6)
    return (wide * scale * gain.astype(jnp.float32)).astype(jnp.bfloat16)


def _place(s_ref, pieces, w_s, unit):
    for n, piece in enumerate(pieces):
        w_s[pl.ds(pl.multiple_of(s_ref[n] * unit, unit), piece.shape[0]), :] = piece[...]


def _turned(t, cos, sin):
    t = t.astype(jnp.float32)
    a, b = t[:, : HEAD // 2], t[:, HEAD // 2 :]
    return (a * cos - b * sin).astype(jnp.bfloat16), (b * cos + a * sin).astype(jnp.bfloat16)


def _put_heads(o_ref, h, t, cos, sin, turn, span):
    for n in range(span):
        part = t[:, n * HEAD : (n + 1) * HEAD]
        if turn:
            o_ref[h + n, :, : HEAD // 2], o_ref[h + n, :, HEAD // 2 :] = _turned(part, cos, sin)
        else:
            o_ref[h + n] = part.T


def _products(tasks):
    ahead = tasks[0][0]()
    for n, (_, use) in enumerate(tasks):
        t = ahead.astype(jnp.bfloat16)
        if n + 1 < len(tasks):
            ahead = tasks[n + 1][0]()
        use(t)


def _project(s_ref, a_ref, b_ref, *rest, turn, unit, half, span):
    pieces, rest = rest[:6], rest[6:]
    cos = sin = None
    if turn:
        (cos, sin), rest = rest[:2], rest[2:]
    o_ref, w_ref = rest
    i = pl.program_id(0)

    @pl.when(i == 0)
    def _():
        _place(s_ref, pieces, w_ref, unit)

    def make(from_ref):
        tasks = []
        for h in range(0, o_ref.shape[0], span):
            tasks.append((
                lambda h=h: _dot(from_ref[...], w_ref[:, h * HEAD : (h + span) * HEAD], 1, 0),
                lambda t, h=h: _put_heads(o_ref, h, t, cos[...] if turn else None, sin[...] if turn else None, turn, span),
            ))
        _products(tasks)

    pl.when(i < half)(lambda: make(a_ref))
    pl.when(i >= half)(lambda: make(b_ref))


def project(a, b, weight, core, tables, places, targets, rows=512, span=2):
    pieces, at = weight
    d = a.shape[1]
    heads = HEADS // 2
    unit = d // 8
    tokens = a.shape[0] + b.shape[0]
    half = a.shape[0] // rows
    steps = 2 * half
    turn = tables is not None
    scalars = jnp.concatenate([at, jnp.stack([core]), places, targets]).astype(jnp.int32)
    specs = [
        pl.BlockSpec((rows, d), lambda i, s: (jnp.minimum(i, half - 1), 0)),
        pl.BlockSpec((rows, d), lambda i, s: (jnp.maximum(i - half, 0), 0)),
    ]
    specs += [pl.BlockSpec((p.shape[0], heads * HEAD), lambda i, s: (0, s[6])) for p in pieces]
    given = [a, b, *pieces]
    if turn:
        specs += [pl.BlockSpec((rows, HEAD // 2), lambda i, s: (s[7 + i], 0))] * 2
        given += tables
        out = jax.ShapeDtypeStruct((heads, tokens, HEAD), jnp.bfloat16)
        out_spec = pl.BlockSpec((heads, rows, HEAD), lambda i, s: (0, s[7 + steps + i], 0))
    else:
        out = jax.ShapeDtypeStruct((heads, HEAD, tokens), jnp.bfloat16)
        out_spec = pl.BlockSpec((heads, HEAD, rows), lambda i, s: (0, 0, s[7 + steps + i]))
    return pl.pallas_call(
        functools.partial(_project, turn=turn, unit=unit, half=half, span=span),
        grid_spec=pltpu.PrefetchScalarGridSpec(
            num_scalar_prefetch=1,
            grid=(steps,),
            in_specs=specs,
            out_specs=[out_spec, pl.BlockSpec((d, heads * HEAD), lambda i, s: (0, 0))],
        ),
        out_shape=[out, jax.ShapeDtypeStruct((d, heads * HEAD), jnp.bfloat16)],
        compiler_params=pltpu.CompilerParams(dimension_semantics=("arbitrary",), vmem_limit_bytes=VMEM),
        cost_estimate=pl.CostEstimate(flops=2 * tokens * d * heads * HEAD, transcendentals=0, bytes_accessed=4 * tokens * d),
    )(scalars, *given)


def _remake(s_ref, a_ref, b_ref, wk_ref, wv_ref, cos, sin, k_ref, v_ref, *, half, span):
    i = pl.program_id(0)

    def make(from_ref):
        tasks = []
        for w_ref, o_ref, turn in ((wk_ref, k_ref, True), (wv_ref, v_ref, False)):
            for h in range(0, o_ref.shape[0], span):
                tasks.append((
                    lambda w_ref=w_ref, h=h: _dot(from_ref[...], w_ref[:, h * HEAD : (h + span) * HEAD], 1, 0),
                    lambda t, o_ref=o_ref, h=h, turn=turn: _put_heads(o_ref, h, t, cos[...], sin[...], turn, span),
                ))
        _products(tasks)

    pl.when(i < half)(lambda: make(a_ref))
    pl.when(i >= half)(lambda: make(b_ref))


def remake(a, b, wk, wv, tables, places, rows=512, span=2):
    d, width = wk.shape
    heads = width // HEAD
    tokens = a.shape[0] + b.shape[0]
    half = a.shape[0] // rows
    return pl.pallas_call(
        functools.partial(_remake, half=half, span=span),
        grid_spec=pltpu.PrefetchScalarGridSpec(
            num_scalar_prefetch=1,
            grid=(2 * half,),
            in_specs=[
                pl.BlockSpec((rows, d), lambda i, s: (jnp.minimum(i, half - 1), 0)),
                pl.BlockSpec((rows, d), lambda i, s: (jnp.maximum(i - half, 0), 0)),
            ]
            + [pl.BlockSpec((d, width), lambda i, s: (0, 0))] * 2
            + [pl.BlockSpec((rows, HEAD // 2), lambda i, s: (s[i], 0))] * 2,
            out_specs=[
                pl.BlockSpec((heads, rows, HEAD), lambda i, s: (0, i, 0)),
                pl.BlockSpec((heads, HEAD, rows), lambda i, s: (0, 0, i)),
            ],
        ),
        out_shape=[
            jax.ShapeDtypeStruct((heads, tokens, HEAD), jnp.bfloat16),
            jax.ShapeDtypeStruct((heads, HEAD, tokens), jnp.bfloat16),
        ],
        compiler_params=pltpu.CompilerParams(dimension_semantics=("arbitrary",), vmem_limit_bytes=VMEM),
        cost_estimate=pl.CostEstimate(flops=4 * tokens * d * width, transcendentals=0, bytes_accessed=6 * tokens * d),
    )(places.astype(jnp.int32), a, b, wk, wv, *tables)


def _finish(s_ref, a_ref, b_ref, x_ref, *rest, unit):
    pieces, (o_ref, w_s) = rest[:6], rest[6:]

    @pl.when(pl.program_id(0) == 0)
    def _():
        _place(s_ref, pieces, w_s, unit)

    seen = jnp.concatenate([a_ref[...], b_ref[...]], axis=1)
    wide = 512
    for n in range(0, o_ref.shape[1], wide):
        y = _dot(seen, w_s[:, n : n + wide], 1, 0)
        o_ref[:, n : n + wide] = (x_ref[:, n : n + wide].astype(jnp.float32) + y).astype(o_ref.dtype)


def finish(a, b, x, weight, core, rows=512):
    pieces, at = weight
    tokens, d = x.shape
    unit = d // 8
    at = jnp.where(at // 4 == core, 0, 4) + at % 4
    return pl.pallas_call(
        functools.partial(_finish, unit=unit),
        grid_spec=pltpu.PrefetchScalarGridSpec(
            num_scalar_prefetch=1,
            grid=(tokens // rows,),
            in_specs=[pl.BlockSpec((rows, d // 2), lambda i, s: (i, 0))] * 2
            + [pl.BlockSpec((rows, d), lambda i, s: (i, 0))]
            + [pl.BlockSpec(p.shape, lambda i, s: (0, 0)) for p in pieces],
            out_specs=pl.BlockSpec((rows, d), lambda i, s: (i, 0)),
            scratch_shapes=[pltpu.VMEM((d, d), jnp.bfloat16)],
        ),
        out_shape=jax.ShapeDtypeStruct(x.shape, x.dtype),
        compiler_params=pltpu.CompilerParams(dimension_semantics=("arbitrary",), vmem_limit_bytes=VMEM),
        cost_estimate=pl.CostEstimate(flops=2 * tokens * d * d, transcendentals=0, bytes_accessed=6 * tokens * d),
    )(at.astype(jnp.int32), a, b, x, *pieces)


def _attend(n_ref, q_ref, k_ref, v_ref, *rest, diagonal, carried, final, bq, bk, wide, sub):
    rest = list(rest)
    if carried:
        mix_in, top_in = rest[:2]
        rest = rest[2:]
    outs, (mix_s, top_s, *slots) = rest[:-4], rest[-4:]
    iq, blocks = pl.program_id(1), pl.num_programs(1)
    e = HEAD**-0.5 * LOG2E
    room = ROOM / e
    strips = range(0, bq, wide)
    base = pl.multiple_of(iq * bq, bq)

    def start():
        if carried:
            mix_s[...] = mix_in[0]
            top_s[0:1, :] = top_in[0]
        else:
            mix_s[...] = jnp.zeros_like(mix_s)
            top_s[0:1, :] = jnp.full((1, bq), NEG, jnp.float32)

    def values(first, keys):
        return jnp.concatenate([v_ref[0, :, pl.ds(first, keys)], jnp.ones((8, keys), jnp.bfloat16)], axis=0)

    def weigh(slot, unit):
        at, first, keys = unit
        top = top_s[0:1, at : at + wide]
        for r in range(0, keys, sub):
            n = min(sub, keys - r)
            s = _dot(k_ref[0, pl.ds(first + r, n), :], q_ref[0, at : at + wide, :], 1, 1)
            slots[slot][r : r + n] = jnp.exp2((s - top) * e).astype(jnp.bfloat16)

    def add(slot, unit):
        at, first, keys = unit
        mix_s[:, at : at + wide] += _dot(values(first, keys), slots[slot][:keys], 1, 0)

    def run(units):
        for t in range(len(units) + 1):
            if t < len(units):
                weigh(t % 2, units[t])
            if t > 0:
                add((t - 1) % 2, units[t - 1])

    def own(at):
        s = _dot(k_ref[0, pl.ds(base + at, wide), :], q_ref[0, at : at + wide, :], 1, 1)
        s = jnp.where(lax.broadcasted_iota(jnp.int32, s.shape, 1) >= lax.broadcasted_iota(jnp.int32, s.shape, 0), s, HIDDEN)
        top = s.max(axis=0, keepdims=True) + room
        top_s[0:1, at : at + wide] = top
        mix_s[:, at : at + wide] = _dot(values(base + at, wide), jnp.exp2((s - top) * e).astype(jnp.bfloat16), 1, 0)

    def blockwise():
        start()
        step = 256

        def strip(i, _):
            at = pl.multiple_of(i * step, step)
            cols = pl.ds(at, step)

            def block(j, _):
                first = pl.multiple_of(j * step, step)
                s = _dot(k_ref[0, pl.ds(first, step), :], q_ref[0, cols, :], 1, 1)
                if diagonal:
                    gap = base + at - first
                    s = jnp.where(lax.broadcasted_iota(jnp.int32, s.shape, 1) + gap >= lax.broadcasted_iota(jnp.int32, s.shape, 0), s, HIDDEN)
                old = top_s[0:1, cols]
                top = jnp.maximum(old, s.max(axis=0, keepdims=True) + room)
                top_s[0:1, cols] = top
                weights = jnp.exp2((s - top) * e).astype(jnp.bfloat16)
                mix_s[:, cols] = mix_s[:, cols] * jnp.exp2((old - top) * e) + _dot(values(first, step), weights, 1, 0)

            lax.fori_loop(0, lax.div(base + at, step) + 1 if diagonal else n_ref[0] * (bk // step), block, None)

        lax.fori_loop(0, bq // step, strip, None)

    if diagonal:
        for at in strips:
            own(at)
        run([(at, base, at) for at in reversed(strips) if at])
    else:
        start()
    count = iq * (bq // bk) if diagonal else n_ref[0]
    lax.fori_loop(0, count, lambda j, _: run([(at, pl.multiple_of(j * bk, bk), bk) for at in strips]), None)
    worst = jnp.max(mix_s[HEAD : HEAD + 1, :])
    pl.when(jnp.logical_not(worst <= MOST))(blockwise)
    if final:

        def put(o_ref):
            o_ref[...] = (mix_s[:HEAD, :] * (1 / mix_s[HEAD : HEAD + 1, :])).T.astype(o_ref.dtype)

        pl.when(iq < blocks // 2)(lambda: put(outs[0]))
        pl.when(iq >= blocks // 2)(lambda: put(outs[1]))
    else:
        outs[0][0] = mix_s[...]
        outs[1][0] = top_s[0:1, :]


def attend(q, k, v, count, core, state=None, *, diagonal, final, bq=2048, bk=2048, wide=256, sub=512):
    heads, queries, d = q.shape
    keys = k.shape[1]
    bk = min(bk, keys)
    blocks = queries // bq
    half = blocks // 2

    def block(iq, s):
        return jnp.where(iq < half, (1 - s[1]) * half + iq, s[1] * half + iq - half) if final else iq

    states = [
        pl.BlockSpec((1, HEAD + 8, bq), lambda ih, iq, s: (ih, 0, block(iq, s))),
        pl.BlockSpec((1, 1, bq), lambda ih, iq, s: (ih, 0, block(iq, s))),
    ]
    specs = [
        pl.BlockSpec((1, bq, d), lambda ih, iq, s: (ih, block(iq, s), 0)),
        pl.BlockSpec((1, keys, d), lambda ih, iq, s: (ih, 0, 0)),
        pl.BlockSpec((1, d, keys), lambda ih, iq, s: (ih, 0, 0)),
    ]
    given = [q, k, v]
    if state is not None:
        given += state
        specs += states
    if final:
        outs = [
            pl.BlockSpec((bq, d), lambda ih, iq, s: (jnp.minimum(iq, half - 1), ih)),
            pl.BlockSpec((bq, d), lambda ih, iq, s: (jnp.maximum(iq - half, 0), ih)),
        ]
        shapes = [jax.ShapeDtypeStruct((queries // 2, heads * d), jnp.bfloat16)] * 2
    else:
        outs = states
        shapes = [jax.ShapeDtypeStruct((heads, HEAD + 8, queries), jnp.float32), jax.ShapeDtypeStruct((heads, 1, queries), jnp.float32)]
    scores = heads * queries * keys // (2 if diagonal else 1)
    return pl.pallas_call(
        functools.partial(_attend, diagonal=diagonal, carried=state is not None, final=final, bq=bq, bk=bk, wide=wide, sub=sub),
        grid_spec=pltpu.PrefetchScalarGridSpec(
            num_scalar_prefetch=1,
            grid=(heads, blocks),
            in_specs=specs,
            out_specs=outs,
            scratch_shapes=[pltpu.VMEM((HEAD + 8, bq), jnp.float32), pltpu.VMEM((8, bq), jnp.float32)]
            + [pltpu.VMEM((max(bk, bq) if diagonal else bk, wide), jnp.bfloat16)] * 2,
        ),
        out_shape=shapes,
        compiler_params=pltpu.CompilerParams(dimension_semantics=("arbitrary", "arbitrary"), vmem_limit_bytes=VMEM),
        cost_estimate=pl.CostEstimate(flops=4 * scores * d, transcendentals=scores, bytes_accessed=sum(t.size * t.dtype.itemsize for t in given)),
    )(jnp.stack([count // bk, core]).astype(jnp.int32), *given)


def solution(mesh):
    def step(x, gain, wq, wk, wv, wo):
        own, _ = x.shape
        y, sp = lax.axis_index("dp"), lax.axis_index("sp")
        chip, core = sp // 2, sp % 2
        rows = 512
        per = own // rows

        def cross(w):
            size = w.shape[0] // 2
            part = lax.dynamic_slice_in_dim(w, y * size, size)
            return _send(part, ACROSS_X)

        mine, far_at, far_other = 2 * (2 * chip + core), 2 * (2 * (1 - chip) + core), 2 * (2 * (1 - chip) + 1 - core)
        at_w = jnp.stack([mine, 2 * (2 * chip + 1 - core), far_at + y, far_at + 1 - y, far_other + y, far_other + 1 - y])

        def gather(w, there, other):
            return [w, _send(w, TO_CORE), there, other, _send(there, TO_CORE), _send(other, TO_CORE)], at_w

        after = lax.optimization_barrier

        there = [cross(w) for w in (wk, wv, wq, wo)]
        a = normed(x, gain)
        b = _send(a, TO_CORE)
        other = [_send(t, ACROSS_Y) for t in there[:2]]
        wk = gather(wk, there[0], other[0])
        far, at = [], [sum(CHUNKS[:n]) for n in range(len(CHUNKS))]
        for first, size in zip(at, CHUNKS):
            part = lax.slice_in_dim(a, first, first + size)
            far.append(_send(part, FORWARD))

        half = HEAD // 2
        place = jnp.arange(4 * own)
        angle = place.astype(jnp.float32)[:, None] * THETA ** (-jnp.arange(half, dtype=jnp.float32) / half)
        tables = [jnp.cos(angle), jnp.sin(angle)]

        step_no = jnp.arange(2 * per)
        targets = jnp.where(step_no < per, core * per + step_no, (1 - core) * per + step_no - per)
        places = 2 * chip * per + targets
        k, wk = project(a, b, wk, core, tables, places, targets)
        there[2], other[1], k = after((there[2], other[1], k))
        wv = gather(wv, there[1], other[1])
        other.append(_send(there[2], ACROSS_Y))
        v, wv = project(a, b, wv, core, None, places, targets)
        other[2], v = after((other[2], v))
        wq = gather(wq, there[2], other[2])
        q, _ = project(a, b, wq, core, tables, places, targets)
        far[0], q, k, v = after((far[0], q, k, v))
        near = _send(far[0], SECOND_TO_CORE)
        state = attend(q, k, v, jnp.int32(0), core, diagonal=True, final=False)
        for n, first in enumerate(at):
            size = CHUNKS[n]
            blocks = size // rows
            step_no = jnp.arange(2 * blocks)
            places = jnp.where(step_no < blocks, core * per + step_no, (1 - core) * per + step_no - blocks) + first // rows
            if n == len(at) - 1:
                state, near, there[3] = after((state, near, there[3]))
                other.append(_send(there[3], ACROSS_Y))
            else:
                state, near = after((state, near))
            k, v = remake(far[n], near, wk, wv, tables, places)
            if n == len(at) - 1:
                k, other[3] = after((k, other[3]))
                wo = gather(wo, there[3], other[3])
            else:
                k, far[n + 1] = after((k, far[n + 1]))
                near = _send(far[n + 1], SECOND_TO_CORE)
            state = attend(q, k, v, 2 * size * chip, core, state, diagonal=False, final=n == len(at) - 1)
        theirs, mine = state
        return finish(mine, _send(theirs, TO_CORE), x, wo, core)

    tokens, whole = P(AXES, None), P("sp", None)

    return jax.shard_map(
        step,
        mesh=mesh,
        in_specs=(tokens, P(None), whole, whole, whole, whole),
        out_specs=tokens,
        check_vma=False,
    )
```

```python
import functools

import jax
import jax.numpy as jnp
from jax import lax
from jax.experimental import pallas as pl
from jax.experimental.pallas import tpu as pltpu
from jax.sharding import PartitionSpec as P


HEAD = 256
HEADS = 8
THETA = 10000
NEG = -1e30
HIDDEN = 2 * NEG
LOG2E = 1.4426950408889634
ROOM = 40.0
MOST = 8192.0
VMEM = 60 * 2**20
AXES = ("dp", "sp")
CHUNKS = (1024, 1024)


def _pairs(to, only=lambda y, x, c: True):
    number = lambda y, x, c: y * 4 + x * 2 + c
    return [(number(*p), number(*to(*p))) for p in [(y, x, c) for y in (0, 1) for x in (0, 1) for c in (0, 1)] if only(*p)]


ACROSS_X = _pairs(lambda y, x, c: (y, 1 - x, c))
ACROSS_Y = _pairs(lambda y, x, c: (1 - y, x, c))
TO_CORE = _pairs(lambda y, x, c: (y, x, 1 - c))
FORWARD = _pairs(lambda y, x, c: (y, 1, c), lambda y, x, c: x == 0)
SECOND_TO_CORE = _pairs(lambda y, x, c: (y, x, 1 - c), lambda y, x, c: x == 1)


def _send(t, pairs):
    return lax.ppermute(t, AXES, pairs)


def _dot(a, b, ca, cb):
    return lax.dot_general(a, b, (((ca,), (cb,)), ((), ())), preferred_element_type=jnp.float32)


def normed(x, gain):
    wide = x.astype(jnp.float32)
    scale = lax.rsqrt(jnp.mean(wide * wide, -1, keepdims=True) + 1e-6)
    return (wide * scale * gain.astype(jnp.float32)).astype(jnp.bfloat16)


def _place(s_ref, pieces, w_s, unit):
    for n, piece in enumerate(pieces):
        w_s[pl.ds(pl.multiple_of(s_ref[n] * unit, unit), piece.shape[0]), :] = piece[...]


def _turned(t, cos, sin):
    t = t.astype(jnp.float32)
    a, b = t[:, : HEAD // 2], t[:, HEAD // 2 :]
    return (a * cos - b * sin).astype(jnp.bfloat16), (b * cos + a * sin).astype(jnp.bfloat16)


def _put_heads(o_ref, h, t, cos, sin, turn, span):
    for n in range(span):
        part = t[:, n * HEAD : (n + 1) * HEAD]
        if turn:
            o_ref[h + n, :, : HEAD // 2], o_ref[h + n, :, HEAD // 2 :] = _turned(part, cos, sin)
        else:
            o_ref[h + n] = part.T


def _products(tasks):
    ahead = tasks[0][0]()
    for n, (_, use) in enumerate(tasks):
        t = ahead.astype(jnp.bfloat16)
        if n + 1 < len(tasks):
            ahead = tasks[n + 1][0]()
        use(t)


def _project(s_ref, a_ref, b_ref, *rest, turn, unit, half, span, count):
    pieces, rest = rest[:count], rest[count:]
    cos = sin = None
    if turn:
        (cos, sin), rest = rest[:2], rest[2:]
    o_ref, w_ref = rest
    i = pl.program_id(0)

    @pl.when(i == 0)
    def _():
        _place(s_ref, pieces, w_ref, unit)

    def make(from_ref):
        tasks = []
        for h in range(0, o_ref.shape[0], span):
            tasks.append((
                lambda h=h: _dot(from_ref[...], w_ref[:, h * HEAD : (h + span) * HEAD], 1, 0),
                lambda t, h=h: _put_heads(o_ref, h, t, cos[...] if turn else None, sin[...] if turn else None, turn, span),
            ))
        _products(tasks)

    pl.when(i < half)(lambda: make(a_ref))
    pl.when(i >= half)(lambda: make(b_ref))


def project(a, b, weight, core, tables, places, targets, rows=512, span=2):
    pieces, at = weight
    d = a.shape[1]
    heads = HEADS // 2
    unit = d // 16
    n = len(pieces)
    tokens = a.shape[0] + b.shape[0]
    half = a.shape[0] // rows
    steps = 2 * half
    turn = tables is not None
    scalars = jnp.concatenate([at, jnp.stack([core]), places, targets]).astype(jnp.int32)
    specs = [
        pl.BlockSpec((rows, d), lambda i, s: (jnp.minimum(i, half - 1), 0)),
        pl.BlockSpec((rows, d), lambda i, s: (jnp.maximum(i - half, 0), 0)),
    ]
    specs += [pl.BlockSpec((p.shape[0], heads * HEAD), lambda i, s: (0, s[n])) for p in pieces]
    given = [a, b, *pieces]
    if turn:
        specs += [pl.BlockSpec((rows, HEAD // 2), lambda i, s: (s[n + 1 + i], 0))] * 2
        given += tables
        out = jax.ShapeDtypeStruct((heads, tokens, HEAD), jnp.bfloat16)
        out_spec = pl.BlockSpec((heads, rows, HEAD), lambda i, s: (0, s[n + 1 + steps + i], 0))
    else:
        out = jax.ShapeDtypeStruct((heads, HEAD, tokens), jnp.bfloat16)
        out_spec = pl.BlockSpec((heads, HEAD, rows), lambda i, s: (0, 0, s[n + 1 + steps + i]))
    return pl.pallas_call(
        functools.partial(_project, turn=turn, unit=unit, half=half, span=span, count=n),
        grid_spec=pltpu.PrefetchScalarGridSpec(
            num_scalar_prefetch=1,
            grid=(steps,),
            in_specs=specs,
            out_specs=[out_spec, pl.BlockSpec((d, heads * HEAD), lambda i, s: (0, 0))],
        ),
        out_shape=[out, jax.ShapeDtypeStruct((d, heads * HEAD), jnp.bfloat16)],
        compiler_params=pltpu.CompilerParams(dimension_semantics=("arbitrary",), vmem_limit_bytes=VMEM),
        cost_estimate=pl.CostEstimate(flops=2 * tokens * d * heads * HEAD, transcendentals=0, bytes_accessed=4 * tokens * d),
    )(scalars, *given)


def _remake(s_ref, a_ref, b_ref, wk_ref, wv_ref, cos, sin, k_ref, v_ref, *, half, span):
    i = pl.program_id(0)

    def make(from_ref):
        tasks = []
        for w_ref, o_ref, turn in ((wk_ref, k_ref, True), (wv_ref, v_ref, False)):
            for h in range(0, o_ref.shape[0], span):
                tasks.append((
                    lambda w_ref=w_ref, h=h: _dot(from_ref[...], w_ref[:, h * HEAD : (h + span) * HEAD], 1, 0),
                    lambda t, o_ref=o_ref, h=h, turn=turn: _put_heads(o_ref, h, t, cos[...], sin[...], turn, span),
                ))
        _products(tasks)

    pl.when(i < half)(lambda: make(a_ref))
    pl.when(i >= half)(lambda: make(b_ref))


def remake(a, b, wk, wv, tables, places, rows=512, span=2):
    d, width = wk.shape
    heads = width // HEAD
    tokens = a.shape[0] + b.shape[0]
    half = a.shape[0] // rows
    return pl.pallas_call(
        functools.partial(_remake, half=half, span=span),
        grid_spec=pltpu.PrefetchScalarGridSpec(
            num_scalar_prefetch=1,
            grid=(2 * half,),
            in_specs=[
                pl.BlockSpec((rows, d), lambda i, s: (jnp.minimum(i, half - 1), 0)),
                pl.BlockSpec((rows, d), lambda i, s: (jnp.maximum(i - half, 0), 0)),
            ]
            + [pl.BlockSpec((d, width), lambda i, s: (0, 0))] * 2
            + [pl.BlockSpec((rows, HEAD // 2), lambda i, s: (s[i], 0))] * 2,
            out_specs=[
                pl.BlockSpec((heads, rows, HEAD), lambda i, s: (0, i, 0)),
                pl.BlockSpec((heads, HEAD, rows), lambda i, s: (0, 0, i)),
            ],
        ),
        out_shape=[
            jax.ShapeDtypeStruct((heads, tokens, HEAD), jnp.bfloat16),
            jax.ShapeDtypeStruct((heads, HEAD, tokens), jnp.bfloat16),
        ],
        compiler_params=pltpu.CompilerParams(dimension_semantics=("arbitrary",), vmem_limit_bytes=VMEM),
        cost_estimate=pl.CostEstimate(flops=4 * tokens * d * width, transcendentals=0, bytes_accessed=6 * tokens * d),
    )(places.astype(jnp.int32), a, b, wk, wv, *tables)


def _finish(s_ref, a_ref, b_ref, x_ref, *rest, unit):
    pieces, (o_ref, w_s) = rest[:6], rest[6:]

    @pl.when(pl.program_id(0) == 0)
    def _():
        _place(s_ref, pieces, w_s, unit)

    seen = jnp.concatenate([a_ref[...], b_ref[...]], axis=1)
    wide = 512
    for n in range(0, o_ref.shape[1], wide):
        y = _dot(seen, w_s[:, n : n + wide], 1, 0)
        o_ref[:, n : n + wide] = (x_ref[:, n : n + wide].astype(jnp.float32) + y).astype(o_ref.dtype)


def finish(a, b, x, weight, core, rows=512):
    pieces, at = weight
    tokens, d = x.shape
    unit = d // 16
    at = jnp.where(at // 8 == core, 0, 8) + at % 8
    return pl.pallas_call(
        functools.partial(_finish, unit=unit),
        grid_spec=pltpu.PrefetchScalarGridSpec(
            num_scalar_prefetch=1,
            grid=(tokens // rows,),
            in_specs=[pl.BlockSpec((rows, d // 2), lambda i, s: (i, 0))] * 2
            + [pl.BlockSpec((rows, d), lambda i, s: (i, 0))]
            + [pl.BlockSpec(p.shape, lambda i, s: (0, 0)) for p in pieces],
            out_specs=pl.BlockSpec((rows, d), lambda i, s: (i, 0)),
            scratch_shapes=[pltpu.VMEM((d, d), jnp.bfloat16)],
        ),
        out_shape=jax.ShapeDtypeStruct(x.shape, x.dtype),
        compiler_params=pltpu.CompilerParams(dimension_semantics=("arbitrary",), vmem_limit_bytes=VMEM),
        cost_estimate=pl.CostEstimate(flops=2 * tokens * d * d, transcendentals=0, bytes_accessed=6 * tokens * d),
    )(at.astype(jnp.int32), a, b, x, *pieces)


def _attend(n_ref, q_ref, k_ref, v_ref, *rest, diagonal, carried, final, bq, bk, wide, sub):
    rest = list(rest)
    if carried:
        mix_in, top_in = rest[:2]
        rest = rest[2:]
    outs, (mix_s, top_s, *slots) = rest[:-4], rest[-4:]
    iq = pl.program_id(1)
    e = HEAD**-0.5 * LOG2E
    room = ROOM / e
    strips = range(0, bq, wide)
    base = pl.multiple_of(iq * bq, bq)

    def start():
        if carried:
            mix_s[...] = mix_in[0]
            top_s[0:1, :] = top_in[0]
        else:
            mix_s[...] = jnp.zeros_like(mix_s)
            top_s[0:1, :] = jnp.full((1, bq), NEG, jnp.float32)

    def values(first, keys):
        return jnp.concatenate([v_ref[0, :, pl.ds(first, keys)], jnp.ones((8, keys), jnp.bfloat16)], axis=0)

    def weigh(slot, unit):
        at, first, keys = unit
        top = top_s[0:1, at : at + wide]
        for r in range(0, keys, sub):
            n = min(sub, keys - r)
            s = _dot(k_ref[0, pl.ds(first + r, n), :], q_ref[0, at : at + wide, :], 1, 1)
            slots[slot][r : r + n] = jnp.exp2((s - top) * e).astype(jnp.bfloat16)

    def add(slot, unit):
        at, first, keys = unit
        mix_s[:, at : at + wide] += _dot(values(first, keys), slots[slot][:keys], 1, 0)

    def run(units):
        for t in range(len(units) + 1):
            if t < len(units):
                weigh(t % 2, units[t])
            if t > 0:
                add((t - 1) % 2, units[t - 1])

    def own(at):
        s = _dot(k_ref[0, pl.ds(base + at, wide), :], q_ref[0, at : at + wide, :], 1, 1)
        s = jnp.where(lax.broadcasted_iota(jnp.int32, s.shape, 1) >= lax.broadcasted_iota(jnp.int32, s.shape, 0), s, HIDDEN)
        top = s.max(axis=0, keepdims=True) + room
        top_s[0:1, at : at + wide] = top
        mix_s[:, at : at + wide] = _dot(values(base + at, wide), jnp.exp2((s - top) * e).astype(jnp.bfloat16), 1, 0)

    def blockwise():
        start()
        step = 256

        def strip(i, _):
            at = pl.multiple_of(i * step, step)
            cols = pl.ds(at, step)

            def block(j, _):
                first = pl.multiple_of(j * step, step)
                s = _dot(k_ref[0, pl.ds(first, step), :], q_ref[0, cols, :], 1, 1)
                if diagonal:
                    gap = base + at - first
                    s = jnp.where(lax.broadcasted_iota(jnp.int32, s.shape, 1) + gap >= lax.broadcasted_iota(jnp.int32, s.shape, 0), s, HIDDEN)
                old = top_s[0:1, cols]
                top = jnp.maximum(old, s.max(axis=0, keepdims=True) + room)
                top_s[0:1, cols] = top
                weights = jnp.exp2((s - top) * e).astype(jnp.bfloat16)
                mix_s[:, cols] = mix_s[:, cols] * jnp.exp2((old - top) * e) + _dot(values(first, step), weights, 1, 0)

            lax.fori_loop(0, lax.div(base + at, step) + 1 if diagonal else n_ref[0] * (bk // step), block, None)

        lax.fori_loop(0, bq // step, strip, None)

    if diagonal:
        for at in strips:
            own(at)
        run([(at, base, at) for at in reversed(strips) if at])
    else:
        start()
    count = iq * (bq // bk) if diagonal else n_ref[0]
    lax.fori_loop(0, count, lambda j, _: run([(at, pl.multiple_of(j * bk, bk), bk) for at in strips]), None)
    worst = jnp.max(mix_s[HEAD : HEAD + 1, :])
    pl.when(jnp.logical_not(worst <= MOST))(blockwise)
    if final:

        outs[0][...] = (mix_s[:HEAD, :] * (1 / mix_s[HEAD : HEAD + 1, :])).T.astype(outs[0].dtype)
    else:
        outs[0][0] = mix_s[...]
        outs[1][0] = top_s[0:1, :]


def attend(q, k, v, count, part, state=None, *, diagonal=False, final=False, bq=2048, bk=2048, wide=256, sub=512):
    heads, queries, d = q.shape
    keys = k.shape[1]
    bk = min(bk, keys)
    blocks = 1 if final else queries // bq

    def block(iq, s):
        return s[1] if final else iq

    states = [
        pl.BlockSpec((1, HEAD + 8, bq), lambda ih, iq, s: (ih, 0, block(iq, s))),
        pl.BlockSpec((1, 1, bq), lambda ih, iq, s: (ih, 0, block(iq, s))),
    ]
    specs = [
        pl.BlockSpec((1, bq, d), lambda ih, iq, s: (ih, block(iq, s), 0)),
        pl.BlockSpec((1, keys, d), lambda ih, iq, s: (ih, 0, 0)),
        pl.BlockSpec((1, d, keys), lambda ih, iq, s: (ih, 0, 0)),
    ]
    given = [q, k, v]
    if state is not None:
        given += state
        specs += states
    if final:
        outs = [pl.BlockSpec((bq, d), lambda ih, iq, s: (0, ih))]
        shapes = [jax.ShapeDtypeStruct((bq, heads * d), jnp.bfloat16)]
    else:
        outs = states
        shapes = [jax.ShapeDtypeStruct((heads, HEAD + 8, queries), jnp.float32), jax.ShapeDtypeStruct((heads, 1, queries), jnp.float32)]
    scores = heads * blocks * bq * keys // (2 if diagonal else 1)
    got = pl.pallas_call(
        functools.partial(_attend, diagonal=diagonal, carried=state is not None, final=final, bq=bq, bk=bk, wide=wide, sub=sub),
        grid_spec=pltpu.PrefetchScalarGridSpec(
            num_scalar_prefetch=1,
            grid=(heads, blocks),
            in_specs=specs,
            out_specs=outs,
            scratch_shapes=[pltpu.VMEM((HEAD + 8, bq), jnp.float32), pltpu.VMEM((8, bq), jnp.float32)]
            + [pltpu.VMEM((max(bk, bq) if diagonal else bk, wide), jnp.bfloat16)] * 2,
        ),
        out_shape=shapes,
        compiler_params=pltpu.CompilerParams(dimension_semantics=("arbitrary", "arbitrary"), vmem_limit_bytes=VMEM),
        cost_estimate=pl.CostEstimate(flops=4 * scores * d, transcendentals=scores, bytes_accessed=sum(t.size * t.dtype.itemsize for t in given)),
    )(jnp.stack([count // bk, part]).astype(jnp.int32), *given)
    return got[0] if final else got


def solution(mesh):
    def step(x, gain, wq, wk, wv, wo):
        own, _ = x.shape
        y, sp = lax.axis_index("dp"), lax.axis_index("sp")
        chip, core = sp // 2, sp % 2
        rows = 512
        per = own // rows

        def cross(w, cuts=1):
            size = w.shape[0] // 2 // cuts
            parts = [lax.dynamic_slice_in_dim(w, y * size * cuts + n * size, size) for n in range(cuts)]
            sent = []
            for part in parts:
                sent.append(_send(part, ACROSS_X))
            return sent

        def hop(there):
            sent = []
            for part in there:
                sent.append(_send(part, ACROSS_Y))
            return sent

        def gather(w, w_core, there, other):
            pieces = [w, w_core, *there, *other] + [_send(t, TO_CORE) for t in (*there, *other[:-1])]
            pieces.append(_send(other[-1], TO_CORE))
            cuts = len(there)
            size = 2 // cuts
            mine, far, far_other = 4 * (2 * chip + core), 4 * (2 * (1 - chip) + core), 4 * (2 * (1 - chip) + 1 - core)
            starts = [mine, 4 * (2 * chip + 1 - core)]
            starts += [first + 2 * half + n * size for first in (far, far_other) for half in (y, 1 - y) for n in range(cuts)]
            return pieces, jnp.stack(starts)

        after = lax.optimization_barrier

        across = [cross(w, cuts) for w, cuts in ((wk, 2), (wv, 1), (wq, 1), (wo, 1))]
        wk_core = _send(wk, TO_CORE)
        a = normed(x, gain)
        b = _send(a, TO_CORE)
        other = [hop(across[0]), hop(across[1])]
        far, at = [], [sum(CHUNKS[:n]) for n in range(len(CHUNKS))]
        for first, size in zip(at, CHUNKS):
            part = lax.slice_in_dim(a, first, first + size)
            far.append(_send(part, FORWARD))

        half = HEAD // 2

        def turns(place):
            angle = place.astype(jnp.float32)[:, None] * THETA ** (-jnp.arange(half, dtype=jnp.float32) / half)
            return [jnp.cos(angle), jnp.sin(angle)]

        tables = turns(2 * chip * own + jnp.arange(2 * own))
        wk = gather(wk, wk_core, across[0], other[0])

        step_no = jnp.arange(2 * per)
        targets = jnp.where(step_no < per, core * per + step_no, (1 - core) * per + step_no - per)
        k, wk = project(a, b, wk, core, tables, targets, targets)
        across[2][0], other[1][0], k = after((across[2][0], other[1][0], k))
        wv = gather(wv, _send(wv, TO_CORE), across[1], other[1])
        other.append(hop(across[2]))
        v, wv = project(a, b, wv, core, None, targets, targets)
        other[2][0], v = after((other[2][0], v))
        wq = gather(wq, _send(wq, TO_CORE), across[2], other[2])
        q, _ = project(a, b, wq, core, tables, targets, targets)
        q, k, v = after((q, k, v))
        state = attend(q, k, v, jnp.int32(0), core, diagonal=True)
        place, far[0], state = after((jnp.arange(2 * own), far[0], state))
        near = _send(far[0], SECOND_TO_CORE)
        tables = turns(place)
        for n, first in enumerate(at):
            size = CHUNKS[n]
            blocks = size // rows
            step_no = jnp.arange(2 * blocks)
            places = jnp.where(step_no < blocks, core * per + step_no, (1 - core) * per + step_no - blocks) + first // rows
            last = n == len(at) - 1
            if last:
                state, near, across[3][0], wo_core = after((state, near, across[3][0], wo_core))
                other.append(hop(across[3]))
            else:
                state, near = after((state, near))
            k, v = remake(far[n], near, wk, wv, tables, places)
            if last:
                k, other[3][0] = after((k, other[3][0]))
                wo = gather(wo, wo_core, across[3], other[3])
            elif n == 0:
                wo_core = _send(wo, TO_CORE)
            if last:
                theirs = attend(q, k, v, 2 * size * chip, 1 - core, list(state), final=True)
                k, theirs = after((k, theirs))
                others = _send(theirs, TO_CORE)
                mine = attend(q, k, v, 2 * size * chip, core, list(state), final=True)
            else:
                state = attend(q, k, v, 2 * size * chip, core, list(state))
                state, far[n + 1] = after((list(state), far[n + 1]))
                near = _send(far[n + 1], SECOND_TO_CORE)
        return finish(mine, others, x, wo, core)

    tokens, whole = P(AXES, None), P("sp", None)

    return jax.shard_map(
        step,
        mesh=mesh,
        in_specs=(tokens, P(None), whole, whole, whole, whole),
        out_specs=tokens,
        check_vma=False,
    )
```

```python
import functools

import jax
import jax.numpy as jnp
from jax import lax
from jax.experimental import pallas as pl
from jax.experimental.pallas import tpu as pltpu
from jax.sharding import PartitionSpec as P


HEAD = 256
HEADS = 8
THETA = 10000
NEG = -1e30
HIDDEN = 2 * NEG
LOG2E = 1.4426950408889634
ROOM = 40.0
MOST = 8192.0
VMEM = 60 * 2**20
AXES = ("dp", "sp")
CHUNKS = (1024, 1024)


def _pairs(to, only=lambda y, x, c: True):
    number = lambda y, x, c: y * 4 + x * 2 + c
    return [(number(*p), number(*to(*p))) for p in [(y, x, c) for y in (0, 1) for x in (0, 1) for c in (0, 1)] if only(*p)]


ACROSS_X = _pairs(lambda y, x, c: (y, 1 - x, c))
ACROSS_Y = _pairs(lambda y, x, c: (1 - y, x, c))
TO_CORE = _pairs(lambda y, x, c: (y, x, 1 - c))
FORWARD = _pairs(lambda y, x, c: (y, 1, c), lambda y, x, c: x == 0)
SECOND_TO_CORE = _pairs(lambda y, x, c: (y, x, 1 - c), lambda y, x, c: x == 1)


def _send(t, pairs):
    return lax.ppermute(t, AXES, pairs)


def _dot(a, b, ca, cb):
    return lax.dot_general(a, b, (((ca,), (cb,)), ((), ())), preferred_element_type=jnp.float32)


def normed(x, gain):
    wide = x.astype(jnp.float32)
    scale = lax.rsqrt(jnp.mean(wide * wide, -1, keepdims=True) + 1e-6)
    return (wide * scale * gain.astype(jnp.float32)).astype(jnp.bfloat16)


def _place(s_ref, pieces, w_s, unit):
    for n, piece in enumerate(pieces):
        w_s[pl.ds(pl.multiple_of(s_ref[n] * unit, unit), piece.shape[0]), :] = piece[...]


def _turned(t, cos, sin):
    t = t.astype(jnp.float32)
    a, b = t[:, : HEAD // 2], t[:, HEAD // 2 :]
    return (a * cos - b * sin).astype(jnp.bfloat16), (b * cos + a * sin).astype(jnp.bfloat16)


def _put_heads(o_ref, h, t, cos, sin, turn, span):
    for n in range(span):
        part = t[:, n * HEAD : (n + 1) * HEAD]
        if turn:
            o_ref[h + n, :, : HEAD // 2], o_ref[h + n, :, HEAD // 2 :] = _turned(part, cos, sin)
        else:
            o_ref[h + n] = part.T


def _products(tasks):
    ahead = tasks[0][0]()
    for n, (_, use) in enumerate(tasks):
        t = ahead.astype(jnp.bfloat16)
        if n + 1 < len(tasks):
            ahead = tasks[n + 1][0]()
        use(t)


def _project(s_ref, a_ref, b_ref, *rest, turn, unit, half, span, count):
    pieces, rest = rest[:count], rest[count:]
    cos = sin = None
    if turn:
        (cos, sin), rest = rest[:2], rest[2:]
    o_ref, w_ref = rest
    i = pl.program_id(0)

    @pl.when(i == 0)
    def _():
        _place(s_ref, pieces, w_ref, unit)

    def make(from_ref):
        tasks = []
        for h in range(0, o_ref.shape[0], span):
            tasks.append((
                lambda h=h: _dot(from_ref[...], w_ref[:, h * HEAD : (h + span) * HEAD], 1, 0),
                lambda t, h=h: _put_heads(o_ref, h, t, cos[...] if turn else None, sin[...] if turn else None, turn, span),
            ))
        _products(tasks)

    pl.when(i < half)(lambda: make(a_ref))
    pl.when(i >= half)(lambda: make(b_ref))


def project(a, b, weight, core, tables, places, targets, rows=512, span=2):
    pieces, at = weight
    d = a.shape[1]
    heads = HEADS // 2
    unit = d // 16
    n = len(pieces)
    tokens = a.shape[0] + b.shape[0]
    half = a.shape[0] // rows
    steps = 2 * half
    turn = tables is not None
    scalars = jnp.concatenate([at, jnp.stack([core]), places, targets]).astype(jnp.int32)
    specs = [
        pl.BlockSpec((rows, d), lambda i, s: (jnp.minimum(i, half - 1), 0)),
        pl.BlockSpec((rows, d), lambda i, s: (jnp.maximum(i - half, 0), 0)),
    ]
    specs += [pl.BlockSpec((p.shape[0], heads * HEAD), lambda i, s: (0, s[n])) for p in pieces]
    given = [a, b, *pieces]
    if turn:
        specs += [pl.BlockSpec((rows, HEAD // 2), lambda i, s: (s[n + 1 + i], 0))] * 2
        given += tables
        out = jax.ShapeDtypeStruct((heads, tokens, HEAD), jnp.bfloat16)
        out_spec = pl.BlockSpec((heads, rows, HEAD), lambda i, s: (0, s[n + 1 + steps + i], 0))
    else:
        out = jax.ShapeDtypeStruct((heads, HEAD, tokens), jnp.bfloat16)
        out_spec = pl.BlockSpec((heads, HEAD, rows), lambda i, s: (0, 0, s[n + 1 + steps + i]))
    return pl.pallas_call(
        functools.partial(_project, turn=turn, unit=unit, half=half, span=span, count=n),
        grid_spec=pltpu.PrefetchScalarGridSpec(
            num_scalar_prefetch=1,
            grid=(steps,),
            in_specs=specs,
            out_specs=[out_spec, pl.BlockSpec((d, heads * HEAD), lambda i, s: (0, 0))],
        ),
        out_shape=[out, jax.ShapeDtypeStruct((d, heads * HEAD), jnp.bfloat16)],
        compiler_params=pltpu.CompilerParams(dimension_semantics=("arbitrary",), vmem_limit_bytes=VMEM),
        cost_estimate=pl.CostEstimate(flops=2 * tokens * d * heads * HEAD, transcendentals=0, bytes_accessed=4 * tokens * d),
    )(scalars, *given)


def _remake(s_ref, a_ref, b_ref, wk_ref, wv_ref, cos, sin, k_ref, v_ref, *, half, span):
    i = pl.program_id(0)

    def make(from_ref):
        tasks = []
        for w_ref, o_ref, turn in ((wk_ref, k_ref, True), (wv_ref, v_ref, False)):
            for h in range(0, o_ref.shape[0], span):
                tasks.append((
                    lambda w_ref=w_ref, h=h: _dot(from_ref[...], w_ref[:, h * HEAD : (h + span) * HEAD], 1, 0),
                    lambda t, o_ref=o_ref, h=h, turn=turn: _put_heads(o_ref, h, t, cos[...], sin[...], turn, span),
                ))
        _products(tasks)

    pl.when(i < half)(lambda: make(a_ref))
    pl.when(i >= half)(lambda: make(b_ref))


def remake(a, b, wk, wv, tables, places, rows=512, span=2):
    d, width = wk.shape
    heads = width // HEAD
    tokens = a.shape[0] + b.shape[0]
    half = a.shape[0] // rows
    return pl.pallas_call(
        functools.partial(_remake, half=half, span=span),
        grid_spec=pltpu.PrefetchScalarGridSpec(
            num_scalar_prefetch=1,
            grid=(2 * half,),
            in_specs=[
                pl.BlockSpec((rows, d), lambda i, s: (jnp.minimum(i, half - 1), 0)),
                pl.BlockSpec((rows, d), lambda i, s: (jnp.maximum(i - half, 0), 0)),
            ]
            + [pl.BlockSpec((d, width), lambda i, s: (0, 0))] * 2
            + [pl.BlockSpec((rows, HEAD // 2), lambda i, s: (s[i], 0))] * 2,
            out_specs=[
                pl.BlockSpec((heads, rows, HEAD), lambda i, s: (0, i, 0)),
                pl.BlockSpec((heads, HEAD, rows), lambda i, s: (0, 0, i)),
            ],
        ),
        out_shape=[
            jax.ShapeDtypeStruct((heads, tokens, HEAD), jnp.bfloat16),
            jax.ShapeDtypeStruct((heads, HEAD, tokens), jnp.bfloat16),
        ],
        compiler_params=pltpu.CompilerParams(dimension_semantics=("arbitrary",), vmem_limit_bytes=VMEM),
        cost_estimate=pl.CostEstimate(flops=4 * tokens * d * width, transcendentals=0, bytes_accessed=6 * tokens * d),
    )(places.astype(jnp.int32), a, b, wk, wv, *tables)


def _finish(s_ref, a_ref, b_ref, x_ref, *rest, unit):
    pieces, (o_ref, w_s) = rest[:6], rest[6:]

    @pl.when(pl.program_id(0) == 0)
    def _():
        _place(s_ref, pieces, w_s, unit)

    seen = jnp.concatenate([a_ref[...], b_ref[...]], axis=1)
    wide = 512
    for n in range(0, o_ref.shape[1], wide):
        y = _dot(seen, w_s[:, n : n + wide], 1, 0)
        o_ref[:, n : n + wide] = (x_ref[:, n : n + wide].astype(jnp.float32) + y).astype(o_ref.dtype)


def finish(a, b, x, weight, core, rows=512):
    pieces, at = weight
    tokens, d = x.shape
    unit = d // 16
    at = jnp.where(at // 8 == core, 0, 8) + at % 8
    return pl.pallas_call(
        functools.partial(_finish, unit=unit),
        grid_spec=pltpu.PrefetchScalarGridSpec(
            num_scalar_prefetch=1,
            grid=(tokens // rows,),
            in_specs=[pl.BlockSpec((rows, d // 2), lambda i, s: (i, 0))] * 2
            + [pl.BlockSpec((rows, d), lambda i, s: (i, 0))]
            + [pl.BlockSpec(p.shape, lambda i, s: (0, 0)) for p in pieces],
            out_specs=pl.BlockSpec((rows, d), lambda i, s: (i, 0)),
            scratch_shapes=[pltpu.VMEM((d, d), jnp.bfloat16)],
        ),
        out_shape=jax.ShapeDtypeStruct(x.shape, x.dtype),
        compiler_params=pltpu.CompilerParams(dimension_semantics=("arbitrary",), vmem_limit_bytes=VMEM),
        cost_estimate=pl.CostEstimate(flops=2 * tokens * d * d, transcendentals=0, bytes_accessed=6 * tokens * d),
    )(at.astype(jnp.int32), a, b, x, *pieces)


def _attend(n_ref, q_ref, k_ref, v_ref, *rest, diagonal, carried, final, bq, bk, wide, sub):
    rest = list(rest)
    if carried:
        mix_in, top_in = rest[:2]
        rest = rest[2:]
    outs, (mix_s, top_s, *slots) = rest[:-4], rest[-4:]
    iq = pl.program_id(1)
    e = HEAD**-0.5 * LOG2E
    room = ROOM / e
    strips = range(0, bq, wide)
    base = pl.multiple_of(iq * bq, bq)

    def start():
        if carried:
            mix_s[...] = mix_in[0]
            top_s[0:1, :] = top_in[0]
        else:
            mix_s[...] = jnp.zeros_like(mix_s)
            top_s[0:1, :] = jnp.full((1, bq), NEG, jnp.float32)

    def values(first, keys):
        return jnp.concatenate([v_ref[0, :, pl.ds(first, keys)], jnp.ones((8, keys), jnp.bfloat16)], axis=0)

    def weigh(slot, unit):
        at, first, keys = unit
        top = top_s[0:1, at : at + wide]
        for r in range(0, keys, sub):
            n = min(sub, keys - r)
            s = _dot(k_ref[0, pl.ds(first + r, n), :], q_ref[0, at : at + wide, :], 1, 1)
            slots[slot][r : r + n] = jnp.exp2((s - top) * e).astype(jnp.bfloat16)

    def add(slot, unit):
        at, first, keys = unit
        mix_s[:, at : at + wide] += _dot(values(first, keys), slots[slot][:keys], 1, 0)

    def run(units):
        for t in range(len(units) + 1):
            if t < len(units):
                weigh(t % 2, units[t])
            if t > 0:
                add((t - 1) % 2, units[t - 1])

    def own(at):
        s = _dot(k_ref[0, pl.ds(base + at, wide), :], q_ref[0, at : at + wide, :], 1, 1)
        s = jnp.where(lax.broadcasted_iota(jnp.int32, s.shape, 1) >= lax.broadcasted_iota(jnp.int32, s.shape, 0), s, HIDDEN)
        top = s.max(axis=0, keepdims=True) + room
        top_s[0:1, at : at + wide] = top
        mix_s[:, at : at + wide] = _dot(values(base + at, wide), jnp.exp2((s - top) * e).astype(jnp.bfloat16), 1, 0)

    def blockwise():
        start()
        step = 256

        def strip(i, _):
            at = pl.multiple_of(i * step, step)
            cols = pl.ds(at, step)

            def block(j, _):
                first = pl.multiple_of(j * step, step)
                s = _dot(k_ref[0, pl.ds(first, step), :], q_ref[0, cols, :], 1, 1)
                if diagonal:
                    gap = base + at - first
                    s = jnp.where(lax.broadcasted_iota(jnp.int32, s.shape, 1) + gap >= lax.broadcasted_iota(jnp.int32, s.shape, 0), s, HIDDEN)
                old = top_s[0:1, cols]
                top = jnp.maximum(old, s.max(axis=0, keepdims=True) + room)
                top_s[0:1, cols] = top
                weights = jnp.exp2((s - top) * e).astype(jnp.bfloat16)
                mix_s[:, cols] = mix_s[:, cols] * jnp.exp2((old - top) * e) + _dot(values(first, step), weights, 1, 0)

            lax.fori_loop(0, lax.div(base + at, step) + 1 if diagonal else n_ref[0] * (bk // step), block, None)

        lax.fori_loop(0, bq // step, strip, None)

    if diagonal:
        for at in strips:
            own(at)
        run([(at, base, at) for at in reversed(strips) if at])
    else:
        start()
    count = iq * (bq // bk) if diagonal else n_ref[0]
    lax.fori_loop(0, count, lambda j, _: run([(at, pl.multiple_of(j * bk, bk), bk) for at in strips]), None)
    worst = jnp.max(mix_s[HEAD : HEAD + 1, :])
    pl.when(jnp.logical_not(worst <= MOST))(blockwise)
    if final:

        outs[0][...] = (mix_s[:HEAD, :] * (1 / mix_s[HEAD : HEAD + 1, :])).T.astype(outs[0].dtype)
    else:
        outs[0][0] = mix_s[...]
        outs[1][0] = top_s[0:1, :]


def attend(q, k, v, count, part, state=None, *, diagonal=False, final=False, bq=2048, bk=2048, wide=256, sub=512):
    heads, queries, d = q.shape
    keys = k.shape[1]
    bk = min(bk, keys)
    blocks = 1 if final else queries // bq

    def block(iq, s):
        return s[1] if final else iq

    states = [
        pl.BlockSpec((1, HEAD + 8, bq), lambda ih, iq, s: (ih, 0, block(iq, s))),
        pl.BlockSpec((1, 1, bq), lambda ih, iq, s: (ih, 0, block(iq, s))),
    ]
    specs = [
        pl.BlockSpec((1, bq, d), lambda ih, iq, s: (ih, block(iq, s), 0)),
        pl.BlockSpec((1, keys, d), lambda ih, iq, s: (ih, 0, 0)),
        pl.BlockSpec((1, d, keys), lambda ih, iq, s: (ih, 0, 0)),
    ]
    given = [q, k, v]
    if state is not None:
        given += state
        specs += states
    if final:
        outs = [pl.BlockSpec((bq, d), lambda ih, iq, s: (0, ih))]
        shapes = [jax.ShapeDtypeStruct((bq, heads * d), jnp.bfloat16)]
    else:
        outs = states
        shapes = [jax.ShapeDtypeStruct((heads, HEAD + 8, queries), jnp.float32), jax.ShapeDtypeStruct((heads, 1, queries), jnp.float32)]
    scores = heads * blocks * bq * keys // (2 if diagonal else 1)
    got = pl.pallas_call(
        functools.partial(_attend, diagonal=diagonal, carried=state is not None, final=final, bq=bq, bk=bk, wide=wide, sub=sub),
        grid_spec=pltpu.PrefetchScalarGridSpec(
            num_scalar_prefetch=1,
            grid=(heads, blocks),
            in_specs=specs,
            out_specs=outs,
            scratch_shapes=[pltpu.VMEM((HEAD + 8, bq), jnp.float32), pltpu.VMEM((8, bq), jnp.float32)]
            + [pltpu.VMEM((max(bk, bq) if diagonal else bk, wide), jnp.bfloat16)] * 2,
        ),
        out_shape=shapes,
        compiler_params=pltpu.CompilerParams(dimension_semantics=("arbitrary", "arbitrary"), vmem_limit_bytes=VMEM),
        cost_estimate=pl.CostEstimate(flops=4 * scores * d, transcendentals=scores, bytes_accessed=sum(t.size * t.dtype.itemsize for t in given)),
    )(jnp.stack([count // bk, part]).astype(jnp.int32), *given)
    return got[0] if final else got


def solution(mesh):
    def step(x, gain, wq, wk, wv, wo):
        own, _ = x.shape
        y, sp = lax.axis_index("dp"), lax.axis_index("sp")
        chip, core = sp // 2, sp % 2
        rows = 512
        per = own // rows

        def cross(w, cuts=1):
            size = w.shape[0] // 2 // cuts
            parts = [lax.dynamic_slice_in_dim(w, y * size * cuts + n * size, size) for n in range(cuts)]
            sent = []
            for part in parts:
                sent.append(_send(part, ACROSS_X))
            return sent

        def hop(there):
            sent = []
            for part in there:
                sent.append(_send(part, ACROSS_Y))
            return sent

        def gather(w, w_core, there, other):
            pieces = [w, w_core, *there, *other] + [_send(t, TO_CORE) for t in (*there, *other[:-1])]
            pieces.append(_send(other[-1], TO_CORE))
            cuts = len(there)
            size = 2 // cuts
            mine, far, far_other = 4 * (2 * chip + core), 4 * (2 * (1 - chip) + core), 4 * (2 * (1 - chip) + 1 - core)
            starts = [mine, 4 * (2 * chip + 1 - core)]
            starts += [first + 2 * half + n * size for first in (far, far_other) for half in (y, 1 - y) for n in range(cuts)]
            return pieces, jnp.stack(starts)

        after = lax.optimization_barrier

        across = [cross(w, cuts) for w, cuts in ((wk, 2), (wv, 1), (wq, 1), (wo, 1))]
        wk_core = _send(wk, TO_CORE)
        a = normed(x, gain)
        b = _send(a, TO_CORE)
        other = [hop(across[0]), hop(across[1])]
        far, at = [], [sum(CHUNKS[:n]) for n in range(len(CHUNKS))]
        for first, size in zip(at, CHUNKS):
            part = lax.slice_in_dim(a, first, first + size)
            far.append(_send(part, FORWARD))

        half = HEAD // 2

        def turns(place):
            angle = place.astype(jnp.float32)[:, None] * THETA ** (-jnp.arange(half, dtype=jnp.float32) / half)
            return [jnp.cos(angle), jnp.sin(angle)]

        tables = turns(2 * chip * own + jnp.arange(2 * own))
        wk = gather(wk, wk_core, across[0], other[0])

        step_no = jnp.arange(2 * per)
        targets = jnp.where(step_no < per, core * per + step_no, (1 - core) * per + step_no - per)
        k, wk = project(a, b, wk, core, tables, targets, targets)
        across[2][0], other[1][0], k = after((across[2][0], other[1][0], k))
        wv = gather(wv, _send(wv, TO_CORE), across[1], other[1])
        other.append(hop(across[2]))
        v, wv = project(a, b, wv, core, None, targets, targets)
        other[2][0], v = after((other[2][0], v))
        wq = gather(wq, _send(wq, TO_CORE), across[2], other[2])
        q, _ = project(a, b, wq, core, tables, targets, targets)
        q, k, v = after((q, k, v))
        state = attend(q, k, v, jnp.int32(0), core, diagonal=True)
        place, far[0], state = after((jnp.arange(2 * own), far[0], state))
        near = _send(far[0], SECOND_TO_CORE)
        tables = turns(place)
        for n, first in enumerate(at):
            size = CHUNKS[n]
            blocks = size // rows
            step_no = jnp.arange(2 * blocks)
            places = jnp.where(step_no < blocks, core * per + step_no, (1 - core) * per + step_no - blocks) + first // rows
            last = n == len(at) - 1
            if last:
                state, near, wo_core = after((state, near, wo_core))
            else:
                state, near = after((state, near))
            k, v = remake(far[n], near, wk, wv, tables, places)
            if last:
                k, across[3][0] = after((k, across[3][0]))
                other.append(hop(across[3]))
            elif n == 0:
                wo_core = _send(wo, TO_CORE)
            if last:
                theirs = attend(q, k, v, 2 * size * chip, 1 - core, list(state), final=True)
                k, theirs, other[3][0] = after((k, theirs, other[3][0]))
                others = _send(theirs, TO_CORE)
                wo = gather(wo, wo_core, across[3], other[3])
                mine = attend(q, k, v, 2 * size * chip, core, list(state), final=True)
            else:
                state = attend(q, k, v, 2 * size * chip, core, list(state))
                state, far[n + 1] = after((list(state), far[n + 1]))
                near = _send(far[n + 1], SECOND_TO_CORE)
        return finish(mine, others, x, wo, core)

    tokens, whole = P(AXES, None), P("sp", None)

    return jax.shard_map(
        step,
        mesh=mesh,
        in_specs=(tokens, P(None), whole, whole, whole, whole),
        out_specs=tokens,
        check_vma=False,
    )
```
